32 devices in a mesh: gx: 4 (over y, x), gy: 8 (over z, core).
Axes of the slice: x: 2, y: 2, z: 4, core: 2. Of those that a mesh axis runs over, the one named last changes fastest.
Arguments:
- velocity: float32 [3, 48, 224, 1024], P(None, 'gx', 'gy'), may hold values from -12 to 12
- viscosity: float32 [48, 224, 1024], P('gx', 'gy'), may hold values from 0.5 to 4
- cells: int32 [3, 32768], P(None, ('gx', 'gy')), may hold values from 0 to 1023, as said below
- offsets: float32 [3, 32768], P(None, ('gx', 'gy')), may hold values from 0 to 1
- forces: float32 [3, 32768], P(None, ('gx', 'gy')), may hold values from -48 to 48
- owners: int32 [32768, 1], P(('gx', 'gy')), may hold values from 0 to 31; in each aligned block of 1024 rows (0 to 1023, 1024 to 2047, ...) at most 64 rows name the same one
Outputs:
- new_velocity: float32 [3, 48, 224, 1024], P(None, 'gx', 'gy')
- marker_velocity: float32 [3, 32768], P(None, ('gx', 'gy'))
The draws below stay inside these ranges and needn't reach their ends.
Inputs may be any that keep to these rules, and one draw needn't show every extreme that they name: cells[0] lies below 12, cells[1] below 28, cells[2] below 1024. `owners`: among one device's 1024 markers at most 64 have the same owner, and in every draw some owner is named exactly 64 times by one device's markers.
All inputs are finite; a program needn't handle non-finite values.
Results may differ from the reference program's by a relative error of at most 0.000096.
Values sent between devices are 32-bit elements; how exact they have to be, the bound alone decides.
A program may use at most 128 MiB of HBM per device.

```python
import math
import jax
import jax.numpy as jnp
import numpy as np

CX = 12
CY = 28
NZ = 1024
M_DEV = 1024
SWEEPS = 3
NX = 48
NY = 224
MARKERS = 32768
CAP = 64
N_GY = 8
DEVICES = 32


def draw_cells(key, part):
    upper = jnp.array([[CX], [CY], [NZ]], jnp.int32)
    return jax.random.randint(key, (3, MARKERS), 0, upper, dtype=jnp.int32)


def block_levels(own_key, extent, cuts, smallest, largest):
    loudness, own = 1.0, jax.random.fold_in(own_key, 6)
    for axis_at, blocks in cuts:
        draws = jnp.exp(jax.random.uniform(jax.random.fold_in(own, axis_at), (blocks,), jnp.float32, smallest / len(cuts), largest / len(cuts)))
        loudness = loudness * jnp.repeat(draws, extent[axis_at] // blocks).reshape([-1 if axis == axis_at else 1 for axis in range(len(extent))])
    return loudness


def assign_block(key, own, number, rows, amount, top, bound, skew):
    order = jax.random.permutation(key, amount)
    heavy_load, ordinary = portions_of(amount, rows * top, bound, skew, True), portions_of(amount, rows * top, bound, skew, False)
    places = jnp.arange(amount)

    def named(tallies, turn):
        used = int((tallies > 0).sum())
        fixed = max(1, used // 4)
        moved = fixed + (places - fixed + turn * (used - fixed)) % max(1, amount - fixed)
        return jnp.zeros((amount,), jnp.int32).at[order[jnp.where(places < fixed, places, moved)]].set(jnp.asarray(tallies, jnp.int32))

    tallies = jnp.where(number % 4 == 0, named(heavy_load, number // 4), named(ordinary, number - number // 4 - 1))
    mixed = jax.random.permutation(jax.random.fold_in(own, 3), amount)
    donor, taker = mixed[0:amount // 2 * 2:2], mixed[1:amount // 2 * 2:2]
    margin = jnp.minimum(tallies[donor] - 1, bound - tallies[taker]) // 2
    margin = jnp.where((donor == order[0]) | (taker == order[0]) | (tallies[taker] == 0), 0, jnp.maximum(margin, 0))
    moved = jax.random.randint(jax.random.fold_in(own, 4), (amount // 2,), 0, 1 << 20) % (margin + 1)
    tallies = tallies.at[donor].add(-moved).at[taker].add(moved)
    labels = jnp.searchsorted(jnp.cumsum(tallies), jnp.arange(rows * top), side="right").astype(jnp.int32)
    grid = labels.reshape(top, rows).T
    grid = grid[jax.random.permutation(jax.random.fold_in(own, 1), rows)]
    turn = jax.random.randint(jax.random.fold_in(own, 2), (rows, 1), 0, top)
    return jnp.take_along_axis(grid, (jnp.arange(top)[None, :] + turn) % top, axis=1)


def portions_of(count, total, limit, slope, full):
    weights = [(1 << 20) // math.isqrt(grade ** slope) + 1 for grade in range(1, count + 1)]
    largest = limit if full else min(limit, max(-(-total // count), total * weights[0] // sum(weights)))
    least = 1 if total - largest >= count - 1 else 0
    counts, rest = [largest] + [least] * (count - 1), total - largest - least * (count - 1)
    while rest > 0:
        free = [i for i in range(1, count) if counts[i] < largest] or [i for i in range(1, count) if counts[i] < limit]
        whole, left = sum([weights[i] for i in free]), rest
        for i in free:
            more = min(limit - counts[i], max(1, left * weights[i] // whole), rest)
            counts[i] = counts[i] + more
            rest = rest - more
    return np.array(counts)


def bell_draw(key, shape, spread, reach, cuts=(), kind=jnp.bfloat16):
    level = block_levels(key, shape, cuts, -0.22, 0.18) if cuts else 1.0
    drawn = jax.random.normal(key, shape, jnp.float32) * spread * level
    return jnp.minimum(jnp.maximum(drawn, -reach), reach).astype(kind)


def setup_inputs(seed: int = 0) -> dict:
    key_of = jax.random.split(jax.random.key(seed), 7)
    velocity = bell_draw(key_of[0], (3, NX, NY, NZ), 2.0, 12.0, ((1, 4), (2, 8)), jnp.float32)
    viscosity = jnp.clip(jnp.exp(math.log(4.0) - 2.0794415 * jax.random.uniform(key_of[1], (NX, NY, NZ), jnp.float32) ** block_levels(key_of[1], (NX, NY, NZ), ((0, 4), (1, 8)), -0.2, 0.2)), 0.5, 4.0)
    cells = draw_cells(jax.random.fold_in(key_of[6], 71), 0)
    offsets = jnp.clip(1.0 * jax.random.uniform(key_of[3], (3, MARKERS), jnp.float32) ** block_levels(key_of[3], (3, MARKERS), ((1, 32),), -0.2, 0.2), 0.0, 1.0)
    forces = bell_draw(key_of[4], (3, MARKERS), 8.0, 48.0, ((1, 32),), jnp.float32)
    owners_keys = jax.random.split(jax.random.fold_in(key_of[5], 1), MARKERS // M_DEV)
    owners_turns = jax.random.permutation(jax.random.fold_in(key_of[5], 3), MARKERS // M_DEV)
    owners = jax.vmap(lambda own, number: assign_block(jax.random.fold_in(key_of[5], 2), own, number, M_DEV, DEVICES, 1, CAP, 2))(owners_keys, owners_turns).reshape((MARKERS, 1))
    return dict(velocity=velocity, viscosity=viscosity, cells=cells, offsets=offsets, forces=forces, owners=owners)


def kernel_weights(frac):
    root = jnp.sqrt(1.0 + 4.0 * frac - 4.0 * frac * frac)
    return jnp.stack([(3.0 - 2.0 * frac - root) / 8.0, (3.0 - 2.0 * frac + root) / 8.0, (1.0 + 2.0 * frac + root) / 8.0, (1.0 + 2.0 * frac - root) / 8.0])

def reference(velocity, viscosity, cells, offsets, forces, owners):
    owner = owners[:, 0]
    base_x = owner // N_GY * CX + cells[0]
    base_y = owner % N_GY * CY + cells[1]
    base_z = cells[2]
    weight_x = kernel_weights(offsets[0])
    weight_y = kernel_weights(offsets[1])
    weight_z = kernel_weights(offsets[2])
    flat = jnp.zeros((3, NX * NY * NZ), jnp.float32)
    entries = []
    for i in range(4):
        for j in range(4):
            for k in range(4):
                index = (((base_x - 1 + i) % NX * NY + (base_y - 1 + j) % NY) * NZ + (base_z - 1 + k) % NZ).astype(jnp.int32)
                weight = weight_x[i] * weight_y[j] * weight_z[k]
                entries.append((index, weight))
                flat = flat.at[:, index].add(forces * weight[None, :])
    rhs = velocity + flat.reshape(3, NX, NY, NZ)
    field = rhs
    for sweep in range(SWEEPS):
        beside_all = jnp.roll(field, -1, 1) + jnp.roll(field, 1, 1)
        beside_all = beside_all + jnp.roll(field, -1, 2) + jnp.roll(field, 1, 2)
        beside_all = beside_all + jnp.roll(field, -1, 3) + jnp.roll(field, 1, 3)
        field = (rhs + viscosity * beside_all) / (1.0 + 6.0 * viscosity)
    values = field.reshape(3, NX * NY * NZ)
    speeds = jnp.zeros((3, owner.shape[0]), jnp.float32)
    for index, weight in entries:
        speeds = speeds + values[:, index] * weight[None, :]
    return (field, speeds)
```

```python
import jax
import jax.numpy as jnp
from jax import lax
from jax.sharding import PartitionSpec as P

SWEEPS = 3


def shifted(block, axis, step):
    count = lax.axis_size(axis)
    return lax.ppermute(block, axis, [(i, (i + step) % count) for i in range(count)])


def cut(block, dim, start, stop):
    return lax.slice_in_dim(block, start, stop, axis=dim)


def kernel_weights(frac):
    root = jnp.sqrt(1.0 + 4.0 * frac - 4.0 * frac * frac)
    return jnp.stack(
        [
            (3.0 - 2.0 * frac - root) / 8.0,
            (3.0 - 2.0 * frac + root) / 8.0,
            (1.0 + 2.0 * frac + root) / 8.0,
            (1.0 + 2.0 * frac - root) / 8.0,
        ]
    )


def tent_table(first, weights, width, periodic):
    columns = lax.broadcasted_iota(jnp.int32, (first.shape[0], width), 1)
    table = jnp.zeros((first.shape[0], width), jnp.float32)
    for j in range(4):
        target = first + j
        if periodic:
            target = jnp.mod(target, width)
        table = table + jnp.where(columns == target[:, None], weights[j][:, None], 0.0)
    return table


def block_tables(received, start, block, ext_x, ext_y, depth):
    part = lax.dynamic_slice_in_dim(received, start, block, 1)
    local_x = part[0].astype(jnp.int32)
    local_y = part[1].astype(jnp.int32)
    local_z = part[2].astype(jnp.int32)
    table_x = tent_table(local_x, kernel_weights(part[3]), ext_x, False)
    table_y = tent_table(local_y - 1, kernel_weights(part[4]), ext_y, True)
    table_z = tent_table(local_z - 1, kernel_weights(part[5]), depth, True)
    planar = (table_x[:, :, None] * table_y[:, None, :]).reshape(block, ext_x * ext_y)
    return (planar, table_z, part)


def neighbour_sum(field):
    size_x, size_y = field.shape[1], field.shape[2]
    x_low = shifted(cut(field, 1, size_x - 1, size_x), "gx", 1)
    x_high = shifted(cut(field, 1, 0, 1), "gx", -1)
    y_low = shifted(cut(field, 2, size_y - 1, size_y), "gy", 1)
    y_high = shifted(cut(field, 2, 0, 1), "gy", -1)
    total = jnp.concatenate([cut(field, 1, 1, size_x), x_high], axis=1)
    total = total + jnp.concatenate([x_low, cut(field, 1, 0, size_x - 1)], axis=1)
    total = total + jnp.concatenate([cut(field, 2, 1, size_y), y_high], axis=2)
    total = total + jnp.concatenate([y_low, cut(field, 2, 0, size_y - 1)], axis=2)
    return total + jnp.roll(field, -1, 3) + jnp.roll(field, 1, 3)


def folded(spread, size_x, size_y):
    ext_y = spread.shape[2]
    y_above = shifted(cut(spread, 2, size_y, size_y + 2), "gy", 1)
    y_below = shifted(cut(spread, 2, ext_y - 1, ext_y), "gy", -1)
    rows = cut(spread, 2, 0, size_y)
    rows = rows + jnp.pad(y_above, ((0, 0), (0, 0), (0, size_y - 2), (0, 0)))
    rows = rows + jnp.pad(y_below, ((0, 0), (0, 0), (size_y - 1, 0), (0, 0)))
    x_above = shifted(cut(rows, 1, size_x + 1, size_x + 3), "gx", 1)
    x_below = shifted(cut(rows, 1, 0, 1), "gx", -1)
    block = cut(rows, 1, 1, size_x + 1)
    block = block + jnp.pad(x_above, ((0, 0), (0, size_x - 2), (0, 0), (0, 0)))
    return block + jnp.pad(x_below, ((0, 0), (size_x - 1, 0), (0, 0), (0, 0)))


def surrounded(field, ext_y):
    size_x, size_y = field.shape[1], field.shape[2]
    x_low = shifted(cut(field, 1, size_x - 1, size_x), "gx", 1)
    x_high = shifted(cut(field, 1, 0, 2), "gx", -1)
    block = jnp.concatenate([x_low, field, x_high], axis=1)
    y_low = shifted(cut(block, 2, size_y - 1, size_y), "gy", 1)
    y_high = shifted(cut(block, 2, 0, 2), "gy", -1)
    spare = jnp.zeros((3, size_x + 3, ext_y - size_y - 3, field.shape[3]), jnp.float32)
    return jnp.concatenate([block, y_high, spare, y_low], axis=2)


def redistribute(payload):
    return lax.all_to_all(payload, ("gx", "gy"), split_axis=1, concat_axis=1, tiled=True)


def shards(velocity, viscosity, cells, offsets, forces, owners):
    rows_gx = lax.axis_size("gx")
    rows_gy = lax.axis_size("gy")
    devices = rows_gx * rows_gy
    markers = owners.shape[0]
    capacity = max(2, 2 * markers // devices)
    slots = capacity * devices
    size_x = velocity.shape[1]
    size_y = velocity.shape[2]
    depth = velocity.shape[3]
    ext_x = size_x + 3
    ext_y = -(-(size_y + 3) // 8) * 8
    owner = owners[:, 0]
    group = min(128, markers)
    onehot = (owner[:, None] == lax.broadcasted_iota(jnp.int32, (markers, devices), 1)).astype(
        jnp.float32
    )
    onehot = onehot.reshape(markers // group, group, devices)
    lower_tri = (
        lax.broadcasted_iota(jnp.int32, (group, group), 0)
        > lax.broadcasted_iota(jnp.int32, (group, group), 1)
    ).astype(jnp.float32)
    within = jnp.einsum("ij,bjd->bid", lower_tri, onehot, precision=lax.Precision.HIGHEST)
    totals = jnp.sum(onehot, axis=1)
    before = jnp.cumsum(totals, axis=0) - totals
    rank = (
        jnp.sum((within + before[:, None, :]) * onehot, axis=-1).reshape(markers).astype(jnp.int32)
    )
    slot = owner * capacity + rank
    payload = jnp.concatenate([cells.astype(jnp.float32), offsets, forces], axis=0)
    outgoing = jnp.zeros((9, slots), jnp.float32).at[:, slot].set(payload)
    received = redistribute(outgoing)
    block = min(512, slots)
    turns = slots // block

    def spread_block(turn, spread):
        planar, table_z, part = block_tables(received, turn * block, block, ext_x, ext_y, depth)
        pushed = part[6:9][:, :, None] * table_z[None, :, :]
        return spread + jnp.einsum("sk,csz->ckz", planar, pushed, precision=lax.Precision.HIGH)

    spread = lax.fori_loop(
        0, turns, spread_block, jnp.zeros((3, ext_x * ext_y, depth), jnp.float32)
    )
    spread = spread.reshape(3, ext_x, ext_y, depth)
    rhs = velocity + folded(spread, size_x, size_y)
    denominator = 1.0 + 6.0 * viscosity
    field = rhs
    for sweep in range(SWEEPS):
        field = (rhs + viscosity * neighbour_sum(field)) / denominator
    field_ext = surrounded(field, ext_y)
    field_flat = field_ext.reshape(3, ext_x * ext_y, depth)

    def sample_block(turn, speeds):
        planar, table_z, part = block_tables(received, turn * block, block, ext_x, ext_y, depth)
        columns = jnp.einsum("sk,ckz->csz", planar, field_flat, precision=lax.Precision.HIGH)
        values = jnp.sum(columns * table_z[None, :, :], axis=-1)
        return lax.dynamic_update_slice_in_dim(speeds, values, turn * block, 1)

    sampled = lax.fori_loop(0, turns, sample_block, jnp.zeros((3, slots), jnp.float32))
    returned = redistribute(sampled)
    marker_velocity = returned[:, slot]
    return (field, marker_velocity)


def solution(mesh):
    in_specs = (
        P(None, "gx", "gy", None),
        P("gx", "gy", None),
        P(None, ("gx", "gy")),
        P(None, ("gx", "gy")),
        P(None, ("gx", "gy")),
        P(("gx", "gy"), None),
    )
    out_specs = (P(None, "gx", "gy", None), P(None, ("gx", "gy")))
    return jax.shard_map(shards, mesh=mesh, in_specs=in_specs, out_specs=out_specs, check_vma=False)
```

```python
import jax
import jax.numpy as jnp
from jax import lax
from jax.experimental import pallas as pl
from jax.experimental.pallas import tpu as pltpu
from jax.sharding import PartitionSpec as P

MESH = pl.DeviceIdType.MESH

SWEEPS = 3


def shifted(block, axis, step):
    count = lax.axis_size(axis)
    return lax.ppermute(block, axis, [(i, (i + step) % count) for i in range(count)])


def cut(block, dim, start, stop):
    return lax.slice_in_dim(block, start, stop, axis=dim)


def kernel_weights(frac):
    root = jnp.sqrt(1.0 + 4.0 * frac - 4.0 * frac * frac)
    return jnp.stack(
        [
            (3.0 - 2.0 * frac - root) / 8.0,
            (3.0 - 2.0 * frac + root) / 8.0,
            (1.0 + 2.0 * frac + root) / 8.0,
            (1.0 + 2.0 * frac - root) / 8.0,
        ]
    )


def tent_table(first, weights, width, periodic):
    columns = lax.broadcasted_iota(jnp.int32, (first.shape[0], width), 1)
    table = jnp.zeros((first.shape[0], width), jnp.float32)
    for j in range(4):
        target = first + j
        if periodic:
            target = jnp.mod(target, width)
        table = table + jnp.where(columns == target[:, None], weights[j][:, None], 0.0)
    return table


def block_tables(received, start, block, ext_x, ext_y, depth):
    part = lax.dynamic_slice_in_dim(received, start, block, 1)
    local_x = part[0].astype(jnp.int32)
    local_y = part[1].astype(jnp.int32)
    local_z = part[2].astype(jnp.int32)
    table_x = tent_table(local_x, kernel_weights(part[3]), ext_x, False)
    table_y = tent_table(local_y - 1, kernel_weights(part[4]), ext_y, True)
    table_z = tent_table(local_z - 1, kernel_weights(part[5]), depth, True)
    planar = (table_x[:, :, None] * table_y[:, None, :]).reshape(block, ext_x * ext_y)
    return (planar, table_z, part)


def folded(spread, size_x, size_y):
    ext_y = spread.shape[2]
    y_above = shifted(cut(spread, 2, size_y, size_y + 2), "gy", 1)
    y_below = shifted(cut(spread, 2, ext_y - 1, ext_y), "gy", -1)
    rows = cut(spread, 2, 0, size_y)
    rows = rows + jnp.pad(y_above, ((0, 0), (0, 0), (0, size_y - 2), (0, 0)))
    rows = rows + jnp.pad(y_below, ((0, 0), (0, 0), (size_y - 1, 0), (0, 0)))
    x_above = shifted(cut(rows, 1, size_x + 1, size_x + 3), "gx", 1)
    x_below = shifted(cut(rows, 1, 0, 1), "gx", -1)
    block = cut(rows, 1, 1, size_x + 1)
    block = block + jnp.pad(x_above, ((0, 0), (0, size_x - 2), (0, 0), (0, 0)))
    return block + jnp.pad(x_below, ((0, 0), (size_x - 1, 0), (0, 0), (0, 0)))


def smoothing_kernel(
    rhs_ref, visc_ref, out_ref, field_a, field_b, x_send, x_recv, x_last_send, x_last,
    y_send, y_recv, y_last_send, y_last_recv, low_send, low_recv, send_sem, recv_sem
):
    size_x, size_y, depth = rhs_ref.shape[1:]
    ext_y = out_ref.shape[2]
    count_x, count_y = lax.axis_size("gx"), lax.axis_size("gy")
    me_x, me_y = lax.axis_index("gx"), lax.axis_index("gy")
    x_up = (lax.rem(me_x + 1, count_x), me_y)
    x_down = (lax.rem(me_x + count_x - 1, count_x), me_y)
    y_up = (me_x, lax.rem(me_y + 1, count_y))
    y_down = (me_x, lax.rem(me_y + count_y - 1, count_y))

    barrier = pltpu.get_barrier_semaphore()
    for device in (x_up, x_down, y_up, y_down):
        pl.semaphore_signal(barrier, inc=1, device_id=device, device_id_type=MESH)
    pl.semaphore_wait(barrier, 4)

    def send(source, target, sem, device):
        copy = pltpu.make_async_remote_copy(
            src_ref=source, dst_ref=target, send_sem=send_sem.at[sem], recv_sem=recv_sem.at[sem],
            device_id=device, device_id_type=MESH,
        )
        copy.start()
        return copy

    def send_x(phase):
        return (
            send(x_send.at[2 * phase], x_recv.at[2 * phase], 4 * phase, x_up),
            send(x_send.at[2 * phase + 1], x_recv.at[2 * phase + 1], 4 * phase + 1, x_down),
        )

    def send_y(phase):
        return (
            send(y_send.at[2 * phase], y_recv.at[2 * phase], 4 * phase + 2, y_up),
            send(y_send.at[2 * phase + 1], y_recv.at[2 * phase + 1], 4 * phase + 3, y_down),
        )

    def pack_y(phase, c, x, plane):
        y_send[2 * phase, x, c : c + 1, :] = plane[size_y - 1 : size_y]
        y_send[2 * phase + 1, x, c : c + 1, :] = plane[0:1]

    def load(x, carry):
        for c in range(3):
            plane = rhs_ref[c, x]
            field_b[c, x, 0:size_y, :] = plane
            pack_y(0, c, x, plane)
        return carry

    load(0, 0)
    load(size_x - 1, 0)
    x_copies = (
        send(rhs_ref.at[:, size_x - 1], x_recv.at[0], 0, x_up),
        send(rhs_ref.at[:, 0], x_recv.at[1], 1, x_down),
    )
    lax.fori_loop(1, size_x - 1, load, 0)
    y_copies = send_y(0)

    for sweep in range(SWEEPS):
        last = sweep == SWEEPS - 1
        current = field_b if sweep % 2 == 0 else field_a
        following = field_a if sweep % 2 == 0 else field_b

        def halo(x, carry):
            for c in range(3):
                current[c, x, size_y : size_y + 1, :] = y_recv[2 * sweep + 1, x, c : c + 1, :]
                current[c, x, ext_y - 1 : ext_y, :] = y_recv[2 * sweep, x, c : c + 1, :]
            return carry

        def update(x, low, high, edge=None):
            visc = visc_ref[x]
            scale = 1.0 / (1.0 + 6.0 * visc)
            for c in range(3):
                wide = current[c, x]
                total = pltpu.roll(wide, 1, 0) + pltpu.roll(wide, ext_y - 1, 0)
                total = total + pltpu.roll(wide, 1, 1) + pltpu.roll(wide, depth - 1, 1)
                total = total[0:size_y] + low(c) + high(c)
                plane = (rhs_ref[c, x] + visc * total) * scale
                if last:
                    out_ref[c, x + 1, 0:size_y, :] = plane
                else:
                    following[c, x, 0:size_y, :] = plane
                    pack_y(sweep + 1, c, x, plane)
                if edge is not None:
                    if last:
                        x_last_send[edge, c] = plane
                    else:
                        x_send[2 * sweep + 2 + edge, c] = plane

        def beside(x):
            return lambda c: current[c, x, 0:size_y, :]

        def interior(x, carry):
            update(x, beside(x - 1), beside(x + 1))
            return carry

        for copy in y_copies:
            copy.wait()
        lax.fori_loop(0, size_x, halo, 0)
        lax.fori_loop(1, size_x - 1, interior, 0)
        for copy in x_copies:
            copy.wait()
        update(0, lambda c: x_recv[2 * sweep, c], beside(1), 1)
        update(size_x - 1, beside(size_x - 2), lambda c: x_recv[2 * sweep + 1, c], 0)
        if not last:
            x_copies = send_x(sweep + 1)
            y_copies = send_y(sweep + 1)

    base = 4 * SWEEPS
    for c in range(3):
        x_last_send[2, c] = out_ref[c, 2, 0:size_y, :]
    x_copies = (
        send(x_last_send.at[0], x_last.at[0], base, x_up),
        send(x_last_send.at[1:3], x_last.at[1:3], base + 1, x_down),
    )

    def pack_last(x, c):
        low_send[x, c : c + 1, :] = out_ref[c, x, size_y - 1 : size_y, :]
        y_last_send[x, 2 * c : 2 * c + 2, :] = out_ref[c, x, 0:2, :]

    def pack_own(x, carry):
        for c in range(3):
            pack_last(x, c)
        return carry

    lax.fori_loop(1, size_x + 1, pack_own, 0)
    for copy in x_copies:
        copy.wait()
    for c in range(3):
        for source, x in enumerate((0, size_x + 1, size_x + 2)):
            out_ref[c, x, 0:size_y, :] = x_last[source, c]
            pack_last(x, c)
    y_copies = (
        send(low_send, low_recv, base + 2, y_up),
        send(y_last_send, y_last_recv, base + 3, y_down),
    )
    for copy in y_copies:
        copy.wait()

    def halo_last(x, carry):
        for c in range(3):
            out_ref[c, x, size_y : ext_y - 1, :] = jnp.zeros((ext_y - 1 - size_y, depth), jnp.float32)
            out_ref[c, x, size_y : size_y + 2, :] = y_last_recv[x, 2 * c : 2 * c + 2, :]
            out_ref[c, x, ext_y - 1 : ext_y, :] = low_recv[x, c : c + 1, :]
        return carry

    lax.fori_loop(0, size_x + 3, halo_last, 0)


def smoothed(rhs, viscosity, ext_y):
    size_x, size_y, depth = viscosity.shape
    ext_x = size_x + 3
    f32 = jnp.float32
    copies = 4 * SWEEPS + 4
    return pl.pallas_call(
        smoothing_kernel,
        out_shape=jax.ShapeDtypeStruct((3, ext_x, ext_y, depth), f32),
        in_specs=[pl.BlockSpec(memory_space=pltpu.VMEM)] * 2,
        out_specs=pl.BlockSpec(memory_space=pltpu.VMEM),
        scratch_shapes=[
            pltpu.VMEM((3, size_x, ext_y, depth), f32),
            pltpu.VMEM((3, size_x, ext_y, depth), f32),
            pltpu.VMEM((2 * SWEEPS, 3, size_y, depth), f32),
            pltpu.VMEM((2 * SWEEPS, 3, size_y, depth), f32),
            pltpu.VMEM((3, 3, size_y, depth), f32),
            pltpu.VMEM((3, 3, size_y, depth), f32),
            pltpu.VMEM((2 * SWEEPS, size_x, 3, depth), f32),
            pltpu.VMEM((2 * SWEEPS, size_x, 3, depth), f32),
            pltpu.VMEM((ext_x, 6, depth), f32),
            pltpu.VMEM((ext_x, 6, depth), f32),
            pltpu.VMEM((ext_x, 3, depth), f32),
            pltpu.VMEM((ext_x, 3, depth), f32),
            pltpu.SemaphoreType.DMA((copies,)),
            pltpu.SemaphoreType.DMA((copies,)),
        ],
        compiler_params=pltpu.CompilerParams(
            collective_id=0, has_side_effects=True, vmem_limit_bytes=56 * 1024 * 1024
        ),
    )(rhs, viscosity)


def redistribute(payload):
    return lax.all_to_all(payload, ("gx", "gy"), split_axis=1, concat_axis=1, tiled=True)


def shards(velocity, viscosity, cells, offsets, forces, owners):
    rows_gx = lax.axis_size("gx")
    rows_gy = lax.axis_size("gy")
    devices = rows_gx * rows_gy
    markers = owners.shape[0]
    capacity = max(2, 2 * markers // devices)
    slots = capacity * devices
    size_x = velocity.shape[1]
    size_y = velocity.shape[2]
    depth = velocity.shape[3]
    ext_x = size_x + 3
    ext_y = -(-(size_y + 3) // 8) * 8
    owner = owners[:, 0]
    group = min(128, markers)
    onehot = (owner[:, None] == lax.broadcasted_iota(jnp.int32, (markers, devices), 1)).astype(
        jnp.float32
    )
    onehot = onehot.reshape(markers // group, group, devices)
    lower_tri = (
        lax.broadcasted_iota(jnp.int32, (group, group), 0)
        > lax.broadcasted_iota(jnp.int32, (group, group), 1)
    ).astype(jnp.float32)
    within = jnp.einsum("ij,bjd->bid", lower_tri, onehot, precision=lax.Precision.HIGHEST)
    totals = jnp.sum(onehot, axis=1)
    before = jnp.cumsum(totals, axis=0) - totals
    rank = (
        jnp.sum((within + before[:, None, :]) * onehot, axis=-1).reshape(markers).astype(jnp.int32)
    )
    slot = owner * capacity + rank
    payload = jnp.concatenate([cells.astype(jnp.float32), offsets, forces], axis=0)
    outgoing = jnp.zeros((9, slots), jnp.float32).at[:, slot].set(payload)
    received = redistribute(outgoing)
    block = min(512, slots)
    turns = slots // block

    def spread_block(turn, spread):
        planar, table_z, part = block_tables(received, turn * block, block, ext_x, ext_y, depth)
        pushed = part[6:9][:, :, None] * table_z[None, :, :]
        return spread + jnp.einsum("sk,csz->ckz", planar, pushed, precision=lax.Precision.HIGH)

    spread = lax.fori_loop(
        0, turns, spread_block, jnp.zeros((3, ext_x * ext_y, depth), jnp.float32)
    )
    spread = spread.reshape(3, ext_x, ext_y, depth)
    rhs = velocity + folded(spread, size_x, size_y)
    field_ext = smoothed(rhs, viscosity, ext_y)
    field = field_ext[:, 1 : size_x + 1, 0:size_y]
    field_flat = field_ext.reshape(3, ext_x * ext_y, depth)

    def sample_block(turn, speeds):
        planar, table_z, part = block_tables(received, turn * block, block, ext_x, ext_y, depth)
        columns = jnp.einsum("sk,ckz->csz", planar, field_flat, precision=lax.Precision.HIGH)
        values = jnp.sum(columns * table_z[None, :, :], axis=-1)
        return lax.dynamic_update_slice_in_dim(speeds, values, turn * block, 1)

    sampled = lax.fori_loop(0, turns, sample_block, jnp.zeros((3, slots), jnp.float32))
    returned = redistribute(sampled)
    marker_velocity = returned[:, slot]
    return (field, marker_velocity)


def solution(mesh):
    in_specs = (
        P(None, "gx", "gy", None),
        P("gx", "gy", None),
        P(None, ("gx", "gy")),
        P(None, ("gx", "gy")),
        P(None, ("gx", "gy")),
        P(("gx", "gy"), None),
    )
    out_specs = (P(None, "gx", "gy", None), P(None, ("gx", "gy")))
    return jax.shard_map(shards, mesh=mesh, in_specs=in_specs, out_specs=out_specs, check_vma=False)
```
